32 devices in a mesh: grp: 8 (over z, y), mem: 4 (over x, core).
Axes of the slice: x: 2, y: 2, z: 4, core: 2. Of those that a mesh axis runs over, the one named last changes fastest.
Arguments:
- queries: bfloat16 [8192, 2048], P(('grp', 'mem')), may hold values from -6 to 6
- keys: bfloat16 [8192, 2048], P(('grp', 'mem')), may hold values from -6 to 6
- values: bfloat16 [8192, 2048], P(('grp', 'mem')), may hold values from -6 to 6
- grad_out: bfloat16 [8192, 2048], P(('grp', 'mem')), may hold values from -0.125 to 0.125
- log_decay: float32 [8, 8192], P(None, ('grp', 'mem')), may hold values from -1.6 to 0
Outputs:
- grad_queries: bfloat16 [8192, 2048], P(('grp', 'mem'))
- grad_keys: bfloat16 [8192, 2048], P(('grp', 'mem'))
- grad_values: bfloat16 [8192, 2048], P(('grp', 'mem'))
The draws below stay inside these ranges and needn't reach their ends.
All inputs are finite; a program needn't handle non-finite values.
Results may differ from the reference program's by a relative error of at most 0.0052.
Values sent between devices are 32-bit elements; how exact they have to be, the bound alone decides.
A program may use at most 128 MiB of HBM per device.

```python
import jax
import jax.numpy as jnp
from jax import lax

HEAD_COUNT = 8
DK = 256
DV = 256
BLOCK = 128
TOK_DEV = 256
SEQUENCE_TOKENS = 8192


def draw_log_decay(key, part):
    base_key = jax.random.fold_in(key, 7)
    key_collection = jax.random.split(base_key, 6)
    order = jax.random.permutation(key_collection[0], HEAD_COUNT)
    fast_count = HEAD_COUNT // 2
    fast = order < fast_count
    fast_rate = jnp.exp(jax.random.uniform(key_collection[1], (HEAD_COUNT,), jnp.float32, jnp.log(1.0 / 50.0), jnp.log(1.0 / 30.0)))
    slow_rate = 0.3 / SEQUENCE_TOKENS
    decay_rates = jnp.where(fast, fast_rate, slow_rate)
    approximate = jnp.exp(jax.random.uniform(key_collection[2], (HEAD_COUNT, SEQUENCE_TOKENS), jnp.float32, jnp.log(0.5), jnp.log(2.0)))
    device_count = SEQUENCE_TOKENS // TOK_DEV
    device_factor = jnp.exp(jax.random.uniform(key_collection[3], (HEAD_COUNT, device_count), jnp.float32, jnp.log(0.5), jnp.log(2.0)))
    device_complete = jnp.repeat(device_factor, TOK_DEV, axis=1)
    spike_start = jax.random.randint(key_collection[4], (HEAD_COUNT, 2), 0, SEQUENCE_TOKENS)
    spike_length = jax.random.uniform(key_collection[5], (HEAD_COUNT, 2), jnp.float32, 0.22, 0.69)
    token_positions = jnp.arange(SEQUENCE_TOKENS)
    match_count = (token_positions[None, None, :] == spike_start[:, :, None]).astype(jnp.float32)
    spike_run = jnp.sum(match_count * spike_length[:, :, None], axis=1)
    return (-(decay_rates[:, None] * approximate * device_complete) - spike_run).astype(jnp.float32)


def block_levels(key, shape, cuts, least, high):
    level = 1.0
    for axis_at, parts in cuts:
        steps = jax.random.uniform(jax.random.fold_in(jax.random.fold_in(key, 6), axis_at), (parts,), jnp.float32, least / len(cuts), high / len(cuts))
        level = level * jnp.repeat(jnp.exp(steps), shape[axis_at] // parts).reshape((-1,) + (1,) * (len(shape) - 1 - axis_at))
    return level


def gaussian(stream_key, extent, scale, limit, pieces=(), kind=jnp.bfloat16):
    gain = block_levels(stream_key, extent, pieces, -0.22, 0.18) if pieces else 1.0
    values = jax.random.normal(stream_key, extent, jnp.float32) * scale * gain
    return jnp.minimum(jnp.maximum(values, -limit), limit).astype(kind)


def setup_inputs(seed: int = 0) -> dict:
    splits = jax.random.split(jax.random.key(seed), 6)
    queries = gaussian(splits[0], (SEQUENCE_TOKENS, HEAD_COUNT * DK), 1.0, 6.0, ((0, 32),))
    keys = gaussian(splits[1], (SEQUENCE_TOKENS, HEAD_COUNT * DK), 1.0, 6.0, ((0, 32),))
    values = gaussian(splits[2], (SEQUENCE_TOKENS, HEAD_COUNT * DV), 1.0, 6.0, ((0, 32),))
    grad_out = gaussian(splits[3], (SEQUENCE_TOKENS, HEAD_COUNT * DV), (2 * SEQUENCE_TOKENS ** -0.5), 0.125, ((0, 32),))
    log_decay = draw_log_decay(jax.random.fold_in(splits[5], 71), 0)
    return dict(queries=queries, keys=keys, values=values, grad_out=grad_out, log_decay=log_decay)


def block_factors(logs):
    cumul = jnp.cumsum(logs, axis=-1)
    ends = cumul[:, -1]
    width = logs.shape[-1]
    lower = jnp.tril(jnp.ones((width, width), dtype=bool))
    spread = cumul[:, :, None] - cumul[:, None, :]
    decay = jnp.where(lower, jnp.exp(jnp.where(lower, spread, 0.0)), 0.0)
    return cumul, ends, decay


def reference(queries, keys, values, grad_out, log_decay):
    count = SEQUENCE_TOKENS // BLOCK
    scale = DK ** -0.5
    query_blocks = queries.reshape(count, BLOCK, HEAD_COUNT, DK)
    key_blocks = keys.reshape(count, BLOCK, HEAD_COUNT, DK)
    value_blocks = values.reshape(count, BLOCK, HEAD_COUNT, DV)
    grad_blocks = grad_out.reshape(count, BLOCK, HEAD_COUNT, DV)
    log_blocks = jnp.transpose(log_decay.reshape(HEAD_COUNT, count, BLOCK), (1, 0, 2))

    def forward_step(state, inputs):
        query_now, key_now, value_now, grad_now, logs = inputs
        query32 = query_now.astype(jnp.float32)
        key32 = key_now.astype(jnp.float32)
        value32 = value_now.astype(jnp.float32)
        grad32 = grad_now.astype(jnp.float32)
        cumul, ends, decay = block_factors(logs)
        scores = jnp.einsum('the,she->hts', grad32, value32)
        weight_grad = lax.optimization_barrier((scores * decay).astype(jnp.bfloat16))
        inner = jnp.einsum('hts,shd->thd', weight_grad.astype(jnp.float32), key32)
        state_low = lax.optimization_barrier(state.astype(jnp.bfloat16))
        outer = jnp.einsum('the,hde->thd', grad32, state_low.astype(jnp.float32))
        outer = outer * jnp.exp(cumul).T[:, :, None]
        result = (scale * (inner + outer)).astype(jnp.bfloat16)
        tail = jnp.exp(ends[:, None] - cumul).T[:, :, None]
        keys_decayed = lax.optimization_barrier((key32 * tail).astype(jnp.bfloat16))
        update = jnp.einsum('shd,she->hde', keys_decayed.astype(jnp.float32), value32)
        state_next = jnp.exp(ends)[:, None, None] * state + update
        return state_next, result

    def reverse_step(state, inputs):
        query_now, key_now, value_now, grad_now, logs = inputs
        query32 = query_now.astype(jnp.float32)
        key32 = key_now.astype(jnp.float32)
        value32 = value_now.astype(jnp.float32)
        grad32 = grad_now.astype(jnp.float32)
        cumul, ends, decay = block_factors(logs)
        scores = jnp.einsum('the,she->hts', grad32, value32)
        weight_grad = lax.optimization_barrier((scores * decay).astype(jnp.bfloat16))
        attend = jnp.einsum('thd,shd->hts', query32, key32)
        weight_value = lax.optimization_barrier((attend * decay).astype(jnp.bfloat16))
        state_low = lax.optimization_barrier(state.astype(jnp.bfloat16)).astype(jnp.float32)
        tail = jnp.exp(ends[:, None] - cumul).T[:, :, None]
        key_grad = jnp.einsum('hts,thd->shd', weight_grad.astype(jnp.float32), query32)
        key_grad = key_grad + tail * jnp.einsum('she,hde->shd', value32, state_low)
        value_grad = jnp.einsum('hts,the->she', weight_value.astype(jnp.float32), grad32)
        value_grad = value_grad + tail * jnp.einsum('shd,hde->she', key32, state_low)
        queries_decayed = lax.optimization_barrier((query32 * jnp.exp(cumul).T[:, :, None]).astype(jnp.bfloat16))
        update = jnp.einsum('thd,the->hde', queries_decayed.astype(jnp.float32), grad32)
        state_next = jnp.exp(ends)[:, None, None] * state + update
        return state_next, ((scale * key_grad).astype(jnp.bfloat16), (scale * value_grad).astype(jnp.bfloat16))

    inputs = (query_blocks, key_blocks, value_blocks, grad_blocks, log_blocks)
    empty = jnp.zeros((HEAD_COUNT, DK, DV), jnp.float32)
    unused, grad_q = lax.scan(forward_step, empty, inputs)
    unused_too, pair = lax.scan(reverse_step, empty, inputs, reverse=True)
    grad_k, grad_v = pair
    return (grad_q.reshape(SEQUENCE_TOKENS, HEAD_COUNT * DK), grad_k.reshape(SEQUENCE_TOKENS, HEAD_COUNT * DK), grad_v.reshape(SEQUENCE_TOKENS, HEAD_COUNT * DV))
```

```python
import functools

import jax
import jax.numpy as jnp
from jax import lax
from jax.experimental import pallas as pl
from jax.experimental.pallas import tpu as pltpu
from jax.sharding import PartitionSpec as P

HEAD_COUNT = 8
DK = 256
DV = 256
BLOCK = 128
CORES = 2
MESH = pl.DeviceIdType.MESH
F32 = jnp.float32
BF16 = jnp.bfloat16


def dot(a, b, ca, cb):
    return lax.dot_general(a, b, (((ca,), (cb,)), ((), ())), preferred_element_type=F32)


def block_cumul(logs_ref, head, b):
    tile = logs_ref[:, b * BLOCK:(b + 1) * BLOCK]
    pick = lax.broadcasted_iota(jnp.int32, tile.shape, 0) == head
    row = jnp.broadcast_to(
        jnp.sum(jnp.where(pick, tile, 0.0), axis=0, keepdims=True), (8, BLOCK)
    )
    lane = lax.broadcasted_iota(jnp.int32, (8, BLOCK), 1)
    step = 1
    while step < BLOCK:
        row = row + jnp.where(lane >= step, pltpu.roll(row, step, 1), 0.0)
        step *= 2
    return row[0:1, :]


def spread_rows(row):
    flat = jnp.broadcast_to(row, (BLOCK, BLOCK))
    return flat, flat.T


def wide(mat, width):
    return jnp.concatenate([mat] * (width // BLOCK), axis=1)


def totals_kernel(count, logs_ref, q_ref, k_ref, v_ref, g_ref, f_ref, r_ref, d_ref):
    head = pl.program_id(0)
    forward = None
    carried = None
    reverse = []
    for b in range(count):
        rows = slice(b * BLOCK, (b + 1) * BLOCK)
        row = block_cumul(logs_ref, head, b)
        _, cols = spread_rows(row)
        end = row[:, BLOCK - 1:BLOCK]
        tail = wide(jnp.exp(end - cols), DK)
        front = wide(jnp.exp(cols), DK)
        kd = (k_ref[rows, :].astype(F32) * tail).astype(BF16)
        qd = (q_ref[rows, :].astype(F32) * front).astype(BF16)
        part = dot(kd, v_ref[rows, :], 0, 0)
        whole = jnp.broadcast_to(jnp.exp(end), (1, DV))
        forward = part if forward is None else whole * forward + part
        carried = whole if carried is None else carried * whole
        reverse.append((whole, dot(qd, g_ref[rows, :], 0, 0)))
    back = None
    for whole, part in reversed(reverse):
        back = part if back is None else whole * back + part
    f_ref[0] = forward
    r_ref[0] = back
    d_ref[0] = carried


def final_kernel(count, logs_ref, q_ref, k_ref, v_ref, g_ref, s_ref, e_ref, gq_ref, gk_ref, gv_ref):
    head = pl.program_id(0)
    scale = DK ** (-0.5)
    lower = lax.broadcasted_iota(jnp.int32, (BLOCK, BLOCK), 0) >= lax.broadcasted_iota(
        jnp.int32, (BLOCK, BLOCK), 1
    )
    state = s_ref[0]
    saved = []
    for b in range(count):
        rows = slice(b * BLOCK, (b + 1) * BLOCK)
        row = block_cumul(logs_ref, head, b)
        flat, cols = spread_rows(row)
        end = row[:, BLOCK - 1:BLOCK]
        decay = jnp.where(lower, jnp.exp(jnp.where(lower, cols - flat, 0.0)), 0.0)
        tail = wide(jnp.exp(end - cols), DK)
        front = wide(jnp.exp(cols), DK)
        whole = jnp.broadcast_to(jnp.exp(end), (1, DV))
        q, k, v, g = q_ref[rows, :], k_ref[rows, :], v_ref[rows, :], g_ref[rows, :]
        wg = (dot(g, v, 1, 1) * decay).astype(BF16)
        wv = (dot(q, k, 1, 1) * decay).astype(BF16)
        low = state.astype(BF16)
        gq_ref[rows, :] = (scale * (dot(wg, k, 1, 0) + front * dot(g, low, 1, 1))).astype(BF16)
        if b < count - 1:
            kd = (k.astype(F32) * tail).astype(BF16)
            state = whole * state + dot(kd, v, 0, 0)
        saved.append((rows, tail, front, whole, wg, wv))
    grads = e_ref[0]
    for b in reversed(range(count)):
        rows, tail, front, whole, wg, wv = saved[b]
        q, k, v, g = q_ref[rows, :], k_ref[rows, :], v_ref[rows, :], g_ref[rows, :]
        low = grads.astype(BF16)
        gk_ref[rows, :] = (scale * (dot(wg, q, 0, 0) + tail * dot(v, low, 1, 1))).astype(BF16)
        gv_ref[rows, :] = (scale * (dot(wv, g, 0, 0) + tail * dot(k, low, 1, 0))).astype(BF16)
        if b > 0:
            qd = (q.astype(F32) * front).astype(BF16)
            grads = whole * grads + dot(qd, g, 0, 0)


def scan_kernel(
    nx, ny, nz, f_ref, r_ref, d_ref, fo_ref, ro_ref,
    peer_buf, chip_buf, plane_buf, out_buf, ztot, zbuf, acc, ret_buf, back_buf,
    dpeer, dchip, dplane, dtot, dz,
    s_core, r_core, s_plane, r_plane, s_z, r_z, s_ret, r_ret, s_back, r_back,
    s_dc, r_dc, s_dp, r_dp, s_dz, r_dz,
):
    chips = nx * ny
    half = HEAD_COUNT // CORES
    width = DK // chips
    group = max(1, half // 2)
    chunks = [(d, k) for k in range(half // group) for d in range(2)]
    number = {c: n for n, c in enumerate(chunks)}
    grp, mem = lax.axis_index("grp"), lax.axis_index("mem")
    z, y = grp // ny, lax.rem(grp, ny)
    x, core = mem // CORES, lax.rem(mem, CORES)
    chip = y * nx + x
    mate = (grp, x * CORES + 1 - core)

    def chip_id(c):
        return (z * ny + c // nx, lax.rem(c, nx) * CORES + core)

    def z_id(to):
        return (to * ny + y, mem)

    others = [lax.rem(chip + off, chips) for off in range(1, chips)]
    zs = [lax.rem(z + off, nz) for off in range(1, nz)]
    peers = [mate] + [chip_id(c) for c in others] + [z_id(t) for t in zs]
    barrier = pltpu.get_barrier_semaphore()
    for peer in peers:
        pl.semaphore_signal(barrier, inc=1, device_id=peer, device_id_type=MESH)
    pl.semaphore_wait(barrier, len(peers))

    def copy(src, dst, send, recv, device):
        return pltpu.make_async_remote_copy(
            src_ref=src, dst_ref=dst, send_sem=send, recv_sem=recv,
            device_id=device, device_id_type=MESH,
        )

    sent = []

    def go(*args):
        c = copy(*args)
        c.start()
        sent.append(c)

    ins = (f_ref, r_ref)
    outs = (fo_ref, ro_ref)
    mine, theirs = core * half, (1 - core) * half

    def span(k):
        return pl.ds(k * group, group)

    def block(c):
        return pl.ds(pl.multiple_of(c * width, width), width)

    go(d_ref, dpeer, s_dc, r_dc, mate)
    for n, (d, k) in enumerate(chunks):
        go(ins[d].at[pl.ds(theirs + k * group, group)], peer_buf.at[d, span(k)],
           s_core.at[n], r_core.at[n], mate)
    copy(d_ref, dpeer, s_dc, r_dc, mate).wait_recv()
    dchip[...] = d_ref[...] * dpeer[...]
    dplane[chip] = d_ref[...] * dpeer[...]
    for o in others:
        go(dchip, dplane.at[chip], s_dp.at[o], r_dp.at[chip], chip_id(o))
    first = core == 0
    for n, (d, k) in enumerate(chunks):
        copy(peer_buf.at[d, span(k)], peer_buf.at[d, span(k)],
             s_core.at[n], r_core.at[n], mate).wait_recv()
        for j in range(k * group, (k + 1) * group):
            own_d = d_ref[mine + j]
            peer_d = dpeer[mine + j]
            one = jnp.ones_like(own_d)
            if d == 0:
                w_own, w_peer = jnp.where(first, peer_d, one), jnp.where(first, one, own_d)
            else:
                w_own, w_peer = jnp.where(first, one, peer_d), jnp.where(first, own_d, one)
            chip_buf[d, j] = w_own * ins[d][mine + j] + w_peer * peer_buf[d, j]
            plane_buf[chip, d, j] = chip_buf[d, j, block(chip), :]
        for o in others:
            go(chip_buf.at[d, span(k), block(o), :], plane_buf.at[chip, d, span(k)],
               s_plane.at[o, n], r_plane.at[chip, n], chip_id(o))

    for o in others:
        copy(dchip, dplane.at[o], s_dp.at[o], r_dp.at[o], chip_id(o)).wait_recv()
    total = dplane[0]
    for c in range(1, chips):
        total = total * dplane[c]
    dtot[...] = total
    for t in zs:
        go(dtot, dz.at[z], s_dz.at[t], r_dz.at[z], z_id(t))

    zsent = []
    for n, (d, k) in enumerate(chunks):
        for o in others:
            copy(plane_buf.at[o, d, span(k)], plane_buf.at[o, d, span(k)],
                 s_plane.at[o, n], r_plane.at[o, n], chip_id(o)).wait_recv()
        order = range(chips) if d == 0 else range(chips - 1, -1, -1)
        for j in range(k * group, (k + 1) * group):
            running = jnp.zeros((width, DV), F32)
            for c in order:
                out_buf[c, d, j] = running
                running = dplane[c, mine + j] * running + plane_buf[c, d, j]
            ztot[d, j] = running
        for t in zs:
            c = copy(ztot.at[d, span(k)], zbuf.at[z, d, span(k)],
                     s_z.at[t, n], r_z.at[z, n], z_id(t))
            needs = (t > z) if d == 0 else (t < z)
            pl.when(needs)(c.start)
            zsent.append((needs, c))

    for t in zs:
        copy(dtot, dz.at[t], s_dz.at[t], r_dz.at[t], z_id(t)).wait_recv()
    for n, (d, k) in enumerate(chunks):
        acc[span(k)] = jnp.zeros((group, width, DV), F32)
        for t in range(nz) if d == 0 else range(nz - 1, -1, -1):
            @pl.when((t < z) if d == 0 else (t > z))
            def _():
                copy(zbuf.at[t, d, span(k)], zbuf.at[t, d, span(k)],
                     s_z.at[t, n], r_z.at[t, n], z_id(t)).wait_recv()
                for j in range(k * group, (k + 1) * group):
                    acc[j] = dz[t, mine + j] * acc[j] + zbuf[t, d, j]
        order = range(chips) if d == 0 else range(chips - 1, -1, -1)
        for j in range(k * group, (k + 1) * group):
            held = acc[j]
            weight = jnp.ones((1, DV), F32)
            for c in order:
                out_buf[c, d, j] = out_buf[c, d, j] + weight * held
                weight = weight * dplane[c, mine + j]
            ret_buf[d, j, block(chip), :] = out_buf[chip, d, j]
        for o in others:
            go(out_buf.at[o, d, span(k)], ret_buf.at[d, span(k), block(chip), :],
               s_ret.at[o, n], r_ret.at[chip, n], chip_id(o))

    for n, (d, k) in enumerate(chunks):
        for o in others:
            copy(out_buf.at[o, d, span(k)], ret_buf.at[d, span(k), block(o), :],
                 s_ret.at[o, n], r_ret.at[o, n], chip_id(o)).wait_recv()
        near = first if d == 0 else jnp.logical_not(first)
        for j in range(k * group, (k + 1) * group):
            @pl.when(near)
            def _():
                got = ret_buf[d, j]
                outs[d][mine + j] = got
                back_buf[d, j] = d_ref[mine + j] * got + ins[d][mine + j]

            @pl.when(jnp.logical_not(near))
            def _():
                got = ret_buf[d, j]
                back_buf[d, j] = got
                outs[d][mine + j] = dpeer[mine + j] * got + peer_buf[d, j]
        go(back_buf.at[d, span(k)], outs[d].at[pl.ds(mine + k * group, group)],
           s_back.at[n], r_back.at[n], mate)
    for n, (d, k) in enumerate(chunks):
        copy(back_buf.at[d, span(k)], outs[d].at[pl.ds(theirs + k * group, group)],
             s_back.at[n], r_back.at[n], mate).wait_recv()
    for c in sent:
        c.wait_send()
    for needs, c in zsent:
        pl.when(needs)(c.wait_send)


def body(nx, ny, nz, queries, keys, values, grad_out, log_decay):
    tokens = queries.shape[0]
    count = tokens // BLOCK
    chips = nx * ny
    half = HEAD_COUNT // CORES
    width = DK // chips
    state = jax.ShapeDtypeStruct((HEAD_COUNT, DK, DV), F32)
    col = pl.BlockSpec((tokens, DK), lambda h: (0, h))
    logs = pl.BlockSpec((HEAD_COUNT, tokens), lambda h: (0, 0))
    mat = pl.BlockSpec((1, DK, DV), lambda h: (h, 0, 0))
    forward, reverse, decays = pl.pallas_call(
        functools.partial(totals_kernel, count),
        grid=(HEAD_COUNT,),
        out_shape=(state, state, jax.ShapeDtypeStruct((HEAD_COUNT, 1, DV), F32)),
        in_specs=[logs, col, col, col, col],
        out_specs=(mat, mat, pl.BlockSpec((1, 1, DV), lambda h: (h, 0, 0))),
        name="totals",
    )(log_decay, queries, keys, values, grad_out)

    vm = pl.BlockSpec(memory_space=pltpu.VMEM)
    dma = pltpu.SemaphoreType.DMA
    group = max(1, half // 2)
    n = 2 * (half // group)
    both = pltpu.VMEM((2, half, DK, DV), F32)
    rows = pltpu.VMEM((HEAD_COUNT, 1, DV), F32)
    state_from, grads_from = pl.pallas_call(
        functools.partial(scan_kernel, nx, ny, nz),
        out_shape=(state, state),
        in_specs=[vm, vm, vm],
        out_specs=(vm, vm),
        scratch_shapes=[
            both, both,
            pltpu.VMEM((chips, 2, half, width, DV), F32),
            pltpu.VMEM((chips, 2, half, width, DV), F32),
            pltpu.VMEM((2, half, width, DV), F32),
            pltpu.VMEM((nz, 2, half, width, DV), F32),
            pltpu.VMEM((half, width, DV), F32),
            both, both,
            rows, rows,
            pltpu.VMEM((chips, HEAD_COUNT, 1, DV), F32),
            rows,
            pltpu.VMEM((nz, HEAD_COUNT, 1, DV), F32),
            dma((n,)), dma((n,)),
            dma((chips, n)), dma((chips, n)),
            dma((nz, n)), dma((nz, n)),
            dma((chips, n)), dma((chips, n)),
            dma((n,)), dma((n,)),
            dma, dma,
            dma((chips,)), dma((chips,)),
            dma((nz,)), dma((nz,)),
        ],
        compiler_params=pltpu.CompilerParams(collective_id=0, has_side_effects=True),
        name="scan",
    )(forward, reverse, decays)

    out = jax.ShapeDtypeStruct((tokens, HEAD_COUNT * DK), BF16)
    return pl.pallas_call(
        functools.partial(final_kernel, count),
        grid=(HEAD_COUNT,),
        out_shape=(out, out, out),
        in_specs=[logs, col, col, col, col, mat, mat],
        out_specs=(col, col, col),
        name="final",
    )(log_decay, queries, keys, values, grad_out, state_from, grads_from)


def solution(mesh):
    nx = mesh.shape["mem"] // CORES
    ny = nx if mesh.shape["grp"] % nx == 0 else 1
    nz = mesh.shape["grp"] // ny
    tokens = P(("grp", "mem"), None)
    return jax.shard_map(
        functools.partial(body, nx, ny, nz),
        mesh=mesh,
        in_specs=(tokens, tokens, tokens, tokens, P(None, ("grp", "mem"))),
        out_specs=(tokens, tokens, tokens),
        check_vma=False,
    )
```

```python
import functools

import jax
import jax.numpy as jnp
from jax import lax
from jax.experimental import pallas as pl
from jax.experimental.pallas import tpu as pltpu
from jax.sharding import PartitionSpec as P

HEAD_COUNT = 8
DK = 256
DV = 256
BLOCK = 128
CORES = 2
LAG = 3
MESH = pl.DeviceIdType.MESH
F32 = jnp.float32
BF16 = jnp.bfloat16


def dot(a, b, ca, cb):
    return lax.dot_general(a, b, (((ca,), (cb,)), ((), ())), preferred_element_type=F32)


def spread_rows(row):
    flat = jnp.broadcast_to(row, (BLOCK, BLOCK))
    return flat, flat.T


def wide(mat, width):
    return jnp.concatenate([mat] * (width // BLOCK), axis=1)


def retention_kernel(
    nx, ny, nz, logs_ref, q_hbm, k_hbm, v_hbm, g_hbm, gq_ref, gk_ref, gv_ref,
    q_ref, k_ref, v_ref, g_ref, s_in, cum, local, inner, total_buf, from_buf,
    peer_buf, chip_buf, plane_buf, out_buf, ztot, zbuf, acc, ret_buf, back_buf,
    d_ref, dpeer, dchip, dplane, dtot, dz,
    s_core, r_core, s_plane, r_plane, s_z, r_z, s_ret, r_ret, s_back, r_back,
    s_dc, r_dc, s_dp, r_dp, s_dz, r_dz,
):
    count = logs_ref.shape[1] // BLOCK
    scale = DK ** (-0.5)
    chips = nx * ny
    half = HEAD_COUNT // CORES
    width = DK // chips
    chunks = [(d, k) for k in range(half) for d in range(2)]
    grp, mem = lax.axis_index("grp"), lax.axis_index("mem")
    z, y = grp // ny, lax.rem(grp, ny)
    x, core = mem // CORES, lax.rem(mem, CORES)
    chip = y * nx + x
    mate = (grp, x * CORES + 1 - core)

    def chip_id(c):
        return (z * ny + c // nx, lax.rem(c, nx) * CORES + core)

    def z_id(to):
        return (to * ny + y, mem)

    others = [lax.rem(chip + off, chips) for off in range(1, chips)]
    zs = [lax.rem(z + off, nz) for off in range(1, nz)]
    peers = [mate] + [chip_id(c) for c in others] + [z_id(t) for t in zs]
    barrier = pltpu.get_barrier_semaphore()
    for peer in peers:
        pl.semaphore_signal(barrier, inc=1, device_id=peer, device_id_type=MESH)

    def copy(src, dst, send, recv, device):
        return pltpu.make_async_remote_copy(
            src_ref=src, dst_ref=dst, send_sem=send, recv_sem=recv,
            device_id=device, device_id_type=MESH,
        )

    sent = []

    def go(*args):
        c = copy(*args)
        c.start()
        sent.append(c)

    mine, theirs = core * half, (1 - core) * half

    def block(c):
        return pl.ds(pl.multiple_of(c * width, width), width)

    def cols_of(head, size):
        return pl.ds(pl.multiple_of(head * size, size), size)

    def tokens_of(b):
        return pl.ds(b * BLOCK, BLOCK)

    def load(i, head):
        far, near = ((q_hbm, q_ref), (k_hbm, k_ref), (v_hbm, v_ref), (g_hbm, g_ref))[i]
        part = cols_of(head, DK)
        return pltpu.make_async_copy(far.at[:, part], near.at[:, part], s_in.at[i, head])

    for k in range(half):
        for head in (theirs + k, mine + k):
            for i in range(4):
                load(i, head).start()

    carried = None
    for b in range(count):
        row = logs_ref[:, b * BLOCK:(b + 1) * BLOCK]
        lane = lax.broadcasted_iota(jnp.int32, row.shape, 1)
        step = 1
        while step < BLOCK:
            row = row + jnp.where(lane >= step, pltpu.roll(row, step, 1), 0.0)
            step *= 2
        whole = jnp.exp(row[:, BLOCK - 1:BLOCK])
        carried = whole if carried is None else carried * whole
        for h in range(HEAD_COUNT):
            cum[b, h] = row[h:h + 1, :]
    carried = jnp.broadcast_to(carried, (HEAD_COUNT, DV))
    for h in range(HEAD_COUNT):
        d_ref[h] = carried[h:h + 1, :]

    def factors(head, b):
        row = cum[b, head]
        flat, cols = spread_rows(row)
        end = row[:, BLOCK - 1:BLOCK]
        return flat, cols, end

    def totals(head):
        for i in range(4):
            load(i, head).wait()
        forward = None
        reverse = []
        for b in range(count):
            _, cols, end = factors(head, b)
            kd = k_ref[tokens_of(b), cols_of(head, DK)].astype(F32) * wide(jnp.exp(end - cols), DK)
            qd = q_ref[tokens_of(b), cols_of(head, DK)].astype(F32) * wide(jnp.exp(cols), DK)
            whole = jnp.broadcast_to(jnp.exp(end), (1, DV))
            part = dot(kd.astype(BF16), v_ref[tokens_of(b), cols_of(head, DV)], 0, 0)
            if b > 0:
                local[0, b - 1, head] = forward
            forward = part if forward is None else whole * forward + part
            reverse.append(
                (whole, dot(qd.astype(BF16), g_ref[tokens_of(b), cols_of(head, DV)], 0, 0))
            )
        back = None
        for b in reversed(range(count)):
            whole, part = reverse[b]
            if b < count - 1:
                local[1, b, head] = back
            back = part if back is None else whole * back + part
        total_buf[0, head] = forward
        total_buf[1, head] = back

    lower = lax.broadcasted_iota(jnp.int32, (BLOCK, BLOCK), 0) >= lax.broadcasted_iota(
        jnp.int32, (BLOCK, BLOCK), 1
    )

    def intra(head):
        for b in range(count):
            flat, cols, _ = factors(head, b)
            decay = jnp.where(lower, jnp.exp(jnp.where(lower, cols - flat, 0.0)), 0.0)
            q = q_ref[tokens_of(b), cols_of(head, DK)]
            k = k_ref[tokens_of(b), cols_of(head, DK)]
            v = v_ref[tokens_of(b), cols_of(head, DV)]
            g = g_ref[tokens_of(b), cols_of(head, DV)]
            wg = (dot(g, v, 1, 1) * decay).astype(BF16)
            wv = (dot(q, k, 1, 1) * decay).astype(BF16)
            inner[0, head, tokens_of(b), :] = dot(wg, k, 1, 0)
            inner[1, head, tokens_of(b), :] = dot(wg, q, 0, 0)
            inner[2, head, tokens_of(b), :] = dot(wv, g, 0, 0)

    def outer(d, head):
        coming = from_buf[d, head]
        weight = None
        order = range(count) if d == 0 else range(count - 1, -1, -1)
        for step, b in enumerate(order):
            _, cols, end = factors(head, b)
            if step == 0:
                low = coming.astype(BF16)
            else:
                low = (local[d, b - 1 if d == 0 else b, head] + weight * coming).astype(BF16)
            whole = jnp.broadcast_to(jnp.exp(end), (1, DV))
            weight = whole if weight is None else weight * whole
            if d == 0:
                g = g_ref[tokens_of(b), cols_of(head, DV)]
                far = wide(jnp.exp(cols), DK) * dot(g, low, 1, 1)
                near = inner[0, head, tokens_of(b), :]
                gq_ref[tokens_of(b), cols_of(head, DK)] = (scale * (near + far)).astype(BF16)
            else:
                tail = wide(jnp.exp(end - cols), DK)
                k = k_ref[tokens_of(b), cols_of(head, DK)]
                v = v_ref[tokens_of(b), cols_of(head, DV)]
                near = inner[1, head, tokens_of(b), :]
                far = tail * dot(v, low, 1, 1)
                gk_ref[tokens_of(b), cols_of(head, DK)] = (scale * (near + far)).astype(BF16)
                near = inner[2, head, tokens_of(b), :]
                far = tail * dot(k, low, 1, 0)
                gv_ref[tokens_of(b), cols_of(head, DV)] = (scale * (near + far)).astype(BF16)

    first = core == 0

    def join_cores(n, d, j):
        copy(peer_buf.at[d, j], peer_buf.at[d, j], s_core.at[n], r_core.at[n], mate).wait_recv()
        own_d = d_ref[mine + j]
        peer_d = dpeer[mine + j]
        one = jnp.ones_like(own_d)
        if d == 0:
            w_own, w_peer = jnp.where(first, peer_d, one), jnp.where(first, one, own_d)
        else:
            w_own, w_peer = jnp.where(first, one, peer_d), jnp.where(first, own_d, one)
        chip_buf[d, j] = w_own * total_buf[d, mine + j] + w_peer * peer_buf[d, j]
        plane_buf[chip, d, j] = chip_buf[d, j, block(chip), :]
        for o in others:
            go(chip_buf.at[d, j, block(o), :], plane_buf.at[chip, d, j],
               s_plane.at[o, n], r_plane.at[chip, n], chip_id(o))

    for k in range(half):
        totals(theirs + k)
        if k == 0:
            pl.semaphore_wait(barrier, len(peers))
            go(d_ref, dpeer, s_dc, r_dc, mate)
        for d in range(2):
            n = chunks.index((d, k))
            go(total_buf.at[d, theirs + k], peer_buf.at[d, k], s_core.at[n], r_core.at[n], mate)
        totals(mine + k)
        if k == 0:
            copy(d_ref, dpeer, s_dc, r_dc, mate).wait_recv()
            dchip[...] = d_ref[...] * dpeer[...]
            dplane[chip] = d_ref[...] * dpeer[...]
            for o in others:
                go(dchip, dplane.at[chip], s_dp.at[o], r_dp.at[chip], chip_id(o))
        for d in range(2):
            join_cores(chunks.index((d, k)), d, k)

    for o in others:
        copy(dchip, dplane.at[o], s_dp.at[o], r_dp.at[o], chip_id(o)).wait_recv()
    total = dplane[0]
    for c in range(1, chips):
        total = total * dplane[c]
    dtot[...] = total
    for t in zs:
        go(dtot, dz.at[z], s_dz.at[t], r_dz.at[z], z_id(t))

    def add_planes(n, d, j):
        acc[...] = jnp.zeros((width, DV), F32)
        for t in range(nz) if d == 0 else range(nz - 1, -1, -1):
            @pl.when((t < z) if d == 0 else (t > z))
            def _():
                copy(zbuf.at[t, d, j], zbuf.at[t, d, j],
                     s_z.at[t, n], r_z.at[t, n], z_id(t)).wait_recv()
                acc[...] = dz[t, mine + j] * acc[...] + zbuf[t, d, j]
        held = acc[...]
        weight = jnp.ones((1, DV), F32)
        for c in range(chips) if d == 0 else range(chips - 1, -1, -1):
            out_buf[c, d, j] = out_buf[c, d, j] + weight * held
            weight = weight * dplane[c, mine + j]
        ret_buf[d, j, block(chip), :] = out_buf[chip, d, j]
        for o in others:
            go(out_buf.at[o, d, j], ret_buf.at[d, j, block(chip), :],
               s_ret.at[o, n], r_ret.at[chip, n], chip_id(o))

    zsent = []
    for n, (d, j) in enumerate(chunks):
        for o in others:
            copy(plane_buf.at[o, d, j], plane_buf.at[o, d, j],
                 s_plane.at[o, n], r_plane.at[o, n], chip_id(o)).wait_recv()
        running = jnp.zeros((width, DV), F32)
        for c in range(chips) if d == 0 else range(chips - 1, -1, -1):
            out_buf[c, d, j] = running
            running = dplane[c, mine + j] * running + plane_buf[c, d, j]
        ztot[d, j] = running
        for t in zs:
            c = copy(ztot.at[d, j], zbuf.at[z, d, j],
                     s_z.at[t, n], r_z.at[z, n], z_id(t))
            needs = (t > z) if d == 0 else (t < z)
            pl.when(needs)(c.start)
            zsent.append((needs, c))
        for h in range(n, HEAD_COUNT, len(chunks)):
            intra(h)
        if n == LAG - 1:
            for t in zs:
                copy(dtot, dz.at[t], s_dz.at[t], r_dz.at[t], z_id(t)).wait_recv()
        if n >= LAG:
            add_planes(n - LAG, *chunks[n - LAG])
    for n in range(len(chunks) - LAG, len(chunks)):
        add_planes(n, *chunks[n])

    def finish(n, d, j):
        copy(back_buf.at[d, j], from_buf.at[d, theirs + j],
             s_back.at[n], r_back.at[n], mate).wait_recv()
        outer(d, theirs + j)

    for n, (d, j) in enumerate(chunks):
        for o in others:
            copy(out_buf.at[o, d, j], ret_buf.at[d, j, block(o), :],
                 s_ret.at[o, n], r_ret.at[o, n], chip_id(o)).wait_recv()
        near = first if d == 0 else jnp.logical_not(first)

        @pl.when(near)
        def _():
            got = ret_buf[d, j]
            from_buf[d, mine + j] = got
            back_buf[d, j] = d_ref[mine + j] * got + total_buf[d, mine + j]

        @pl.when(jnp.logical_not(near))
        def _():
            got = ret_buf[d, j]
            back_buf[d, j] = got
            from_buf[d, mine + j] = dpeer[mine + j] * got + peer_buf[d, j]

        go(back_buf.at[d, j], from_buf.at[d, mine + j], s_back.at[n], r_back.at[n], mate)
        outer(d, mine + j)
        if n > 0:
            finish(n - 1, *chunks[n - 1])
    finish(len(chunks) - 1, *chunks[-1])
    for c in sent:
        c.wait_send()
    for needs, c in zsent:
        pl.when(needs)(c.wait_send)


def body(nx, ny, nz, queries, keys, values, grad_out, log_decay):
    tokens = queries.shape[0]
    count = tokens // BLOCK
    chips = nx * ny
    half = HEAD_COUNT // CORES
    width = DK // chips
    n = 2 * half
    vm = pl.BlockSpec(memory_space=pltpu.VMEM)
    dma = pltpu.SemaphoreType.DMA
    both = pltpu.VMEM((2, half, DK, DV), F32)
    full = pltpu.VMEM((2, HEAD_COUNT, DK, DV), F32)
    rows = pltpu.VMEM((HEAD_COUNT, 1, DV), F32)
    tok = pltpu.VMEM((tokens, HEAD_COUNT * DK), BF16)
    out = jax.ShapeDtypeStruct((tokens, HEAD_COUNT * DK), BF16)
    return pl.pallas_call(
        functools.partial(retention_kernel, nx, ny, nz),
        out_shape=(out, out, out),
        in_specs=[vm] + [pl.BlockSpec(memory_space=pltpu.HBM)] * 4,
        out_specs=(vm, vm, vm),
        scratch_shapes=[
            tok, tok, tok, tok, dma((4, HEAD_COUNT)),
            pltpu.VMEM((count, HEAD_COUNT, 1, BLOCK), F32),
            pltpu.VMEM((2, max(1, count - 1), HEAD_COUNT, DK, DV), F32),
            pltpu.VMEM((3, HEAD_COUNT, tokens, DK), F32),
            full, full,
            both, both,
            pltpu.VMEM((chips, 2, half, width, DV), F32),
            pltpu.VMEM((chips, 2, half, width, DV), F32),
            pltpu.VMEM((2, half, width, DV), F32),
            pltpu.VMEM((nz, 2, half, width, DV), F32),
            pltpu.VMEM((width, DV), F32),
            both, both,
            rows, rows, rows,
            pltpu.VMEM((chips, HEAD_COUNT, 1, DV), F32),
            rows,
            pltpu.VMEM((nz, HEAD_COUNT, 1, DV), F32),
            dma((n,)), dma((n,)),
            dma((chips, n)), dma((chips, n)),
            dma((nz, n)), dma((nz, n)),
            dma((chips, n)), dma((chips, n)),
            dma((n,)), dma((n,)),
            dma, dma,
            dma((chips,)), dma((chips,)),
            dma((nz,)), dma((nz,)),
        ],
        compiler_params=pltpu.CompilerParams(collective_id=0, has_side_effects=True, vmem_limit_bytes=50 << 20),
        name="retention",
    )(log_decay, queries, keys, values, grad_out)


def solution(mesh):
    nx = mesh.shape["mem"] // CORES
    ny = nx if mesh.shape["grp"] % nx == 0 else 1
    nz = mesh.shape["grp"] // ny
    tokens = P(("grp", "mem"), None)
    return jax.shard_map(
        functools.partial(body, nx, ny, nz),
        mesh=mesh,
        in_specs=(tokens, tokens, tokens, tokens, P(None, ("grp", "mem"))),
        out_specs=(tokens, tokens, tokens),
        check_vma=False,
    )
```
